64 devices in a mesh: dp: 4 (over x, y), tp: 16 (over z, core).
Axes of the slice: x: 2, y: 2, z: 8, core: 2. Of those that a mesh axis runs over, the one named last changes fastest.
The devices are a block of a 4x4x8 slice.
Arguments:
- x: bfloat16 [192, 64, 2560], P('dp'), parts along dimension 0
- g1: float32 [2, 2560], replicated
- g2: float32 [2, 2560], replicated
- wqkv: bfloat16 [2, 2560, 32, 240], P(None, None, 'tp')
- wo: bfloat16 [2, 2560, 2560], P(None, 'tp')
- w1: bfloat16 [2, 2560, 10240], P(None, None, 'tp')
- w2: bfloat16 [2, 10240, 2560], P(None, 'tp')
Outputs:
- output: bfloat16 [192, 64, 2560], P('dp'), parts along dimension 0
There are 4 independent parts. The reference program is written for one: setup_inputs(seed, part) draws one part's arguments, and reference() takes and returns one part's arrays. A program takes and returns all parts, laid end to end along the dimension named above; an argument that names none is the same for every part.
All inputs are finite; a program needn't handle non-finite values.
Results may differ from the reference program's by a relative error of at most 0.02.
Values are sent between devices in bfloat16 or wider.
A program may use at most 768 MiB of HBM per device.

```python
import jax
import jax.numpy as jnp
from jax import lax

BATCH = 48
SEQ = 64
D = 2560
HEADS = 32
FF = 10240
LAYERS = 2

HD = D // HEADS
EPS = 1e-5


def setup_inputs(seed: int = 0, part: int = 0) -> dict:
    kx = jax.random.fold_in(jax.random.key(seed), part)
    k = jax.random.split(jax.random.key(seed + 1), 6)
    x = jax.random.normal(kx, (BATCH, SEQ, D), jnp.float32).astype(jnp.bfloat16)
    g1 = 1.0 + 0.3 * jax.random.normal(k[0], (LAYERS, D), jnp.float32)
    g2 = 1.0 + 0.3 * jax.random.normal(k[1], (LAYERS, D), jnp.float32)
    wqkv = (1.5 * D ** -0.5 * jax.random.normal(k[2], (LAYERS, D, HEADS, 3 * HD), jnp.float32)).astype(jnp.bfloat16)
    wo = (D ** -0.5 * jax.random.normal(k[3], (LAYERS, D, D), jnp.float32)).astype(jnp.bfloat16)
    w1 = (D ** -0.5 * jax.random.normal(k[4], (LAYERS, D, FF), jnp.float32)).astype(jnp.bfloat16)
    w2 = (FF ** -0.5 * jax.random.normal(k[5], (LAYERS, FF, D), jnp.float32)).astype(jnp.bfloat16)
    return {"x": x, "g1": g1, "g2": g2, "wqkv": wqkv, "wo": wo, "w1": w1, "w2": w2}


def _ln(x, g):
    xf = x.astype(jnp.float32)
    mu = jnp.mean(xf, axis=-1, keepdims=True)
    var = jnp.mean(jnp.square(xf - mu), axis=-1, keepdims=True)
    return ((xf - mu) * lax.rsqrt(var + EPS) * g).astype(jnp.bfloat16)


def _attend(item):
    q = item[:, 0]
    k = item[:, 1]
    v = item[:, 2]
    s = jnp.dot(q, k.T, preferred_element_type=jnp.float32) * (HD ** -0.5)
    row = lax.broadcasted_iota(jnp.int32, (SEQ, SEQ), 0)
    col = lax.broadcasted_iota(jnp.int32, (SEQ, SEQ), 1)
    s = jnp.where(row >= col, s, -jnp.inf)
    p = jax.nn.softmax(s, axis=-1).astype(jnp.bfloat16)
    return jnp.dot(p, v, preferred_element_type=jnp.float32).astype(jnp.bfloat16)


def _layer(x, w):
    g1, g2, wqkv, wo, w1, w2 = w
    t = BATCH * SEQ
    h = x.reshape(t, D)
    a = _ln(h, g1)
    qkv = jnp.dot(a, wqkv.reshape(D, 3 * D), preferred_element_type=jnp.float32).astype(jnp.bfloat16)
    qkv = qkv.reshape(BATCH, SEQ, HEADS, 3, HD).transpose(0, 2, 1, 3, 4).reshape(BATCH * HEADS, SEQ, 3, HD)
    o = lax.map(_attend, qkv)
    o = o.reshape(BATCH, HEADS, SEQ, HD).transpose(0, 2, 1, 3).reshape(t, D)
    h = (h.astype(jnp.float32) + jnp.dot(o, wo, preferred_element_type=jnp.float32)).astype(jnp.bfloat16)
    m = jax.nn.gelu(jnp.dot(_ln(h, g2), w1, preferred_element_type=jnp.float32), approximate=True).astype(jnp.bfloat16)
    h = (h.astype(jnp.float32) + jnp.dot(m, w2, preferred_element_type=jnp.float32)).astype(jnp.bfloat16)
    return h.reshape(BATCH, SEQ, D), None


def reference(x, g1, g2, wqkv, wo, w1, w2):
    y, _ = lax.scan(_layer, x, (g1, g2, wqkv, wo, w1, w2))
    return y
```

```python
import functools

import jax
import jax.numpy as jnp
from jax import lax
from jax.experimental import pallas as pl
from jax.experimental.pallas import tpu as pltpu
from jax.sharding import PartitionSpec as P

EPS = 1e-5
MESH = pl.DeviceIdType.MESH
F32 = jnp.float32
BF16 = jnp.bfloat16
VMEM_LIMIT = 62 * 1024 * 1024


def _dot(a, b, ca, cb):
    return lax.dot_general(a, b, (((ca,), (cb,)), ((), ())), preferred_element_type=F32)


def _ln_rows(load, store, g, rows):
    def body(i, _):
        r = pl.ds(pl.multiple_of(i * 16, 16), 16)
        xf = load(r).astype(F32)
        d = xf - jnp.mean(xf, axis=-1, keepdims=True)
        var = jnp.mean(d * d, axis=-1, keepdims=True)
        store(r, (d * lax.rsqrt(var + EPS) * g).astype(BF16))
        return 0

    lax.fori_loop(0, rows // 16, body, 0)


def _place(nz):
    t = lax.axis_index("tp")
    z, c = t // 2, t % 2
    return t, z, c


def _chip(z, c, nz, sign, steps):
    fwd = sign * (1 - 2 * c) * steps
    return ((z + fwd + 8 * nz) % nz) * 2 + c


def _barrier(ids):
    sem = pltpu.get_barrier_semaphore()
    for i in ids:
        pl.semaphore_signal(sem, inc=1, device_id={"tp": i}, device_id_type=MESH)
    pl.semaphore_wait(sem, len(ids))


def _ring_kernel(kind, layer, nz, streams, *refs):
    (x_ref, g_ref, wa_ref, wb_ref, out_ref,
     abuf, pbuf, rbuf, wa, wb, own32, p32, mid, mid2,
     x_sem, w_sem, wsend_sem, wrecv_sem, ag_send, ag_recv, rs_send, rs_recv) = refs
    gather = kind != "att0"
    attention = kind != "mlp"
    t, z, c = _place(nz)
    nxt = [_chip(z, c, nz, sg, 1) for _, _, sg in streams]
    peer = t + 1 - 2 * c
    rows, width = own32.shape
    last = nz - 1

    _barrier([_chip(z, c, nz, 1, 1), _chip(z, c, nz, -1, 1), peer])

    own_w, send_w = [], []
    for i, (src, dst) in enumerate(((wa_ref, wa), (wb_ref, wb))):
        src = src.at[layer]
        if kind == "mlp" and i == 0:
            n = src.shape[1]
            lo, hi = dst.at[:, pl.ds(0, n)], dst.at[:, pl.ds(n, n)]
        else:
            n = src.shape[0]
            lo, hi = dst.at[pl.ds(0, n)], dst.at[pl.ds(n, n)]
        own_w.append(pltpu.make_async_copy(src, lo, w_sem.at[i]))
        send_w.append(pltpu.make_async_remote_copy(
            src_ref=src, dst_ref=hi, send_sem=wsend_sem.at[i], recv_sem=wrecv_sem.at[i],
            device_id={"tp": peer}, device_id_type=MESH))

    def x_copy(k, s):
        r0, nr, sg = streams[k]
        dev = _chip(z, c, nz, -sg, s)
        src = x_ref.at[pl.ds(pl.multiple_of(dev * rows + r0, 32), nr)]
        return pltpu.make_async_copy(src, abuf.at[s, pl.ds(r0, nr)], x_sem.at[k, s])

    def ag_copy(k, s):
        r0, nr, _ = streams[k]
        r = pl.ds(r0, nr)
        return pltpu.make_async_remote_copy(
            src_ref=abuf.at[s, r], dst_ref=abuf.at[s + 1, r], send_sem=ag_send.at[k, s], recv_sem=ag_recv.at[k, s + 1],
            device_id={"tp": nxt[k]}, device_id_type=MESH)

    def rs_copy(k, s):
        r0, nr, _ = streams[k]
        r = pl.ds(r0, nr)
        return pltpu.make_async_remote_copy(
            src_ref=pbuf.at[s, r], dst_ref=rbuf.at[s, r], send_sem=rs_send.at[k, s], recv_sem=rs_recv.at[k, s],
            device_id={"tp": nxt[k]}, device_id_type=MESH)

    ks = range(len(streams))
    g = g_ref[pl.ds(layer, 1), :]
    if not gather:
        for i in range(nz):
            for k in ks:
                x_copy(k, (i + 1) % nz).start()
    for w in own_w + send_w:
        w.start()
    if gather:
        _ln_rows(lambda r: x_ref[r, :], lambda r, v: abuf.__setitem__((0, r), v), g, rows)
        for k in ks:
            ag_copy(k, 0).start()
        own32[...] = x_ref[...].astype(F32)
    for w in own_w:
        w.wait()
    for w in send_w:
        w.wait_recv()

    if attention:
        hd = wb.shape[0] // (2 * 2)
        key = lax.broadcasted_iota(jnp.int32, (rows, rows), 0)
        query = lax.broadcasted_iota(jnp.int32, (rows, rows), 1)
        seq = rows // 3
        visible = (key <= query) & (key // seq == query // seq)

    def partial_sum(s):
        if attention:
            mid[...] = _dot(wa[...], abuf[s], 1, 1).astype(BF16)

            def head(h, _):
                base = h * (3 * hd)
                q = mid[pl.ds(pl.multiple_of(base, 16), hd), :]
                k = mid[pl.ds(pl.multiple_of(base + hd, 16), hd), :]
                v = mid[pl.ds(pl.multiple_of(base + 2 * hd, 16), hd), :]
                sc = _dot(k, q, 0, 0) * (hd ** -0.5)
                sc = jnp.where(visible, sc, -jnp.inf)
                e = jnp.exp(sc - jnp.max(sc, axis=0, keepdims=True))
                p = (e / jnp.sum(e, axis=0, keepdims=True)).astype(BF16)
                mid2[pl.ds(pl.multiple_of(h * hd, 16), hd), :] = _dot(v, p, 1, 0).astype(BF16)
                return 0

            lax.fori_loop(0, 4, head, 0)
            tile = 512

            def cols(n, _):
                cc = pl.ds(pl.multiple_of(n * tile, tile), tile)
                p32[:, cc] = _dot(mid2[...], wb[:, cc], 0, 0)
                return 0

            lax.fori_loop(0, width // tile, cols, 0)
        else:
            t1, t2 = 256, 512

            def hidden(n, _):
                cc = pl.ds(pl.multiple_of(n * t1, t1), t1)
                mid[:, cc] = jax.nn.gelu(_dot(abuf[s], wa[:, cc], 1, 0), approximate=True).astype(BF16)
                return 0

            lax.fori_loop(0, mid.shape[1] // t1, hidden, 0)

            def cols(n, _):
                cc = pl.ds(pl.multiple_of(n * t2, t2), t2)
                p32[:, cc] = _dot(mid[...], wb[:, cc], 1, 0)
                return 0

            lax.fori_loop(0, width // t2, cols, 0)

    def step(i, _):
        s = i if gather else i + ((9 - i) // 8) * (1 - 2 * i)

        if gather:
            @pl.when(s > 0)
            def _():
                for k in ks:
                    ag_copy(k, s - 1).wait_recv()

                    @pl.when(s < last)
                    def _():
                        ag_copy(k, s).start()
        else:
            for k in ks:
                x_copy(k, s).wait()

            @pl.when(s == 0)
            def _():
                own32[...] = abuf[0].astype(F32)

            _ln_rows(lambda r: abuf[s, r], lambda r, v: abuf.__setitem__((s, r), v), g, rows)

        partial_sum(s)

        @pl.when(s == 0)
        def _():
            own32[...] += p32[...]

        @pl.when(s > 0)
        def _():
            for k in ks:
                r0, nr, _ = streams[k]
                r = pl.ds(r0, nr)

                @pl.when(s == 1)
                def _():
                    pbuf[s, r] = p32[r, :].astype(BF16)

                @pl.when(s > 1)
                def _():
                    rs_copy(k, s - 1).wait_recv()
                    pbuf[s, r] = (p32[r, :] + rbuf[s - 1, r].astype(F32)).astype(BF16)

                rs_copy(k, s).start()

        return 0

    lax.fori_loop(0, nz, step, 0)

    for k in ks:
        r0, nr, _ = streams[k]
        r = pl.ds(r0, nr)
        rs_copy(k, last).wait_recv()
        out_ref[r, :] = (own32[r, :] + rbuf[last, r].astype(F32)).astype(BF16)

    def drain(s, _):
        for k in ks:
            rs_copy(k, s).wait_send()
            if gather:
                ag_copy(k, s - 1).wait_send()
        return 0

    lax.fori_loop(1, nz, drain, 0)
    for w in send_w:
        w.wait_send()


def _ring_call(kind, layer, nz, cid, x, g, wa, wb, rows, width):
    fine = ((0, rows // 3, 1), (rows // 3, rows // 3, 1), (2 * rows // 3, rows // 6, -1), (5 * rows // 6, rows // 6, -1))
    coarse = ((0, 2 * rows // 3, 1), (2 * rows // 3, rows // 3, -1))
    streams = fine if kind == "att0" else coarse
    nk = len(streams)
    big = pltpu.VMEM((nz, rows, width), BF16)
    if kind == "mlp":
        wshape = ((width, 2 * wa.shape[2]), (2 * wb.shape[1], width))
        mids = ((rows, 2 * wa.shape[2]), (16, 128))
    else:
        wshape = ((2 * wa.shape[1], width), (2 * wb.shape[1], width))
        mids = ((2 * wa.shape[1], rows), (2 * wb.shape[1], rows))
    vmem, hbm = pl.BlockSpec(memory_space=pltpu.VMEM), pl.BlockSpec(memory_space=pl.ANY)
    dma = pltpu.SemaphoreType.DMA
    return pl.pallas_call(
        functools.partial(_ring_kernel, kind, layer, nz, streams),
        out_shape=jax.ShapeDtypeStruct((rows, width), BF16),
        in_specs=[hbm if kind == "att0" else vmem, vmem, hbm, hbm],
        out_specs=vmem,
        scratch_shapes=[
            big, big, big, pltpu.VMEM(wshape[0], BF16), pltpu.VMEM(wshape[1], BF16),
            pltpu.VMEM((rows, width), F32), pltpu.VMEM((rows, width), F32),
            pltpu.VMEM(mids[0], BF16), pltpu.VMEM(mids[1], BF16),
            dma((nk, nz)), dma((2,)), dma((2,)), dma((2,)),
            dma((nk, nz)), dma((nk, nz)), dma((nk, nz)), dma((nk, nz)),
        ],
        compiler_params=pltpu.CompilerParams(collective_id=cid, has_side_effects=True, vmem_limit_bytes=VMEM_LIMIT),
        name=f"{kind}_{layer}",
    )(x, g, wa, wb)


def _gather_kernel(nz, streams, x_ref, out_ref, buf, loc_sem, send_sem, recv_sem, psend_sem, precv_sem):
    t, z, c = _place(nz)
    nxt = [_chip(z, c, nz, sg, 1) for _, _, sg in streams]
    peer = t + 1 - 2 * c
    rows = x_ref.shape[0]
    ks = range(len(streams))
    last = nz - 1
    _barrier([_chip(z, c, nz, 1, 1), _chip(z, c, nz, -1, 1), peer])

    def src(k, s):
        r0, nr, _ = streams[k]
        return buf.at[s, pl.ds(r0, nr)]

    def spot(k, s, core):
        r0, nr, sg = streams[k]
        dev = _chip(z, core, nz, -sg * (1 - 2 * c) * (1 - 2 * core), s)
        return out_ref.at[pl.ds(pl.multiple_of(dev * rows + r0, 32), nr)]

    def ring(k, s):
        return pltpu.make_async_remote_copy(
            src_ref=src(k, s), dst_ref=src(k, s + 1), send_sem=send_sem.at[k, s], recv_sem=recv_sem.at[k, s + 1],
            device_id={"tp": nxt[k]}, device_id_type=MESH)

    def local(k, s):
        return pltpu.make_async_copy(src(k, s), spot(k, s, c), loc_sem.at[k, s])

    def across(k, s):
        return pltpu.make_async_remote_copy(
            src_ref=src(k, s), dst_ref=spot(k, s, c), send_sem=psend_sem.at[k, s], recv_sem=precv_sem.at[k, s],
            device_id={"tp": peer}, device_id_type=MESH)

    own = pltpu.make_async_copy(x_ref, buf.at[0], loc_sem.at[0, 0])
    own.start()
    own.wait()
    for k in ks:
        ring(k, 0).start()
    for k in ks:
        local(k, 0).start()
        across(k, 0).start()

    def step(s, _):
        for k in ks:
            ring(k, s - 1).wait_recv()

            @pl.when(s < last)
            def _():
                ring(k, s).start()

            local(k, s).start()
            across(k, s).start()
        return 0

    lax.fori_loop(1, nz, step, 0)

    def drain(s, _):
        for k in ks:
            local(k, s).wait()
            across(k, s).wait()

            @pl.when(s < last)
            def _():
                ring(k, s).wait_send()
        return 0

    lax.fori_loop(0, nz, drain, 0)


def _gather_call(nz, cid, x):
    rows, width = x.shape
    streams = ((0, rows // 3, 1), (rows // 3, rows // 3, 1), (2 * rows // 3, rows // 6, -1), (5 * rows // 6, rows // 6, -1))
    nk = len(streams)
    dma = pltpu.SemaphoreType.DMA
    hbm = pl.BlockSpec(memory_space=pl.ANY)
    return pl.pallas_call(
        functools.partial(_gather_kernel, nz, streams),
        out_shape=jax.ShapeDtypeStruct((2 * nz * rows, width), BF16),
        in_specs=[hbm],
        out_specs=hbm,
        scratch_shapes=[pltpu.VMEM((nz, rows, width), BF16)] + [dma((nk, nz))] * 5,
        compiler_params=pltpu.CompilerParams(collective_id=cid, has_side_effects=True, vmem_limit_bytes=VMEM_LIMIT),
        name="gather",
    )(x)


def solution(mesh):
    n = mesh.shape["tp"]
    nz = n // 2

    def body(x, g1, g2, wqkv, wo, w1, w2):
        b, s, d = x.shape
        rows = b * s // n
        layers, _, hl, hd3 = wqkv.shape
        wt = wqkv.transpose(0, 2, 3, 1).reshape(layers, hl * hd3, d)
        h = x.reshape(b * s, d)
        cid = 0
        for l in range(layers):
            h = _ring_call("att0" if l == 0 else "att", l, nz, cid, h, g1, wt, wo, rows, d)
            h = _ring_call("mlp", l, nz, cid + 1, h, g2, w1, w2, rows, d)
            cid += 2
        return _gather_call(nz, cid, h).reshape(b, s, d)

    in_specs = (P("dp"), P(), P(), P(None, None, "tp", None), P(None, "tp", None), P(None, None, "tp"), P(None, "tp", None))
    return jax.shard_map(body, mesh=mesh, in_specs=in_specs, out_specs=P("dp"), check_vma=False)
```

```python
import functools
import math

import jax
import jax.numpy as jnp
from jax import lax
from jax.experimental import pallas as pl
from jax.experimental.pallas import tpu as pltpu
from jax.sharding import PartitionSpec as P

EPS = 1e-5
MESH = pl.DeviceIdType.MESH
F32 = jnp.float32
BF16 = jnp.bfloat16
VMEM_LIMIT = 62 * 1024 * 1024


def _dot(a, b, ca, cb):
    return lax.dot_general(a, b, (((ca,), (cb,)), ((), ())), preferred_element_type=F32)


def _ln_rows(load, store, g, rows):
    def body(i, _):
        r = pl.ds(pl.multiple_of(i * 16, 16), 16)
        xf = load(r).astype(F32)
        d = xf - jnp.mean(xf, axis=-1, keepdims=True)
        var = jnp.mean(d * d, axis=-1, keepdims=True)
        store(r, (d * lax.rsqrt(var + EPS) * g).astype(BF16))
        return 0

    lax.fori_loop(0, rows // 16, body, 0)


def _place(nz):
    t = lax.axis_index("tp")
    z, c = t // 2, t % 2
    return t, z, c


def _chip(z, c, nz, sign, steps):
    fwd = sign * (1 - 2 * c) * steps
    return ((z + fwd + 8 * nz) % nz) * 2 + c


def _barrier(ids, nd=1):
    sem = pltpu.get_barrier_semaphore()
    for i in ids:
        pl.semaphore_signal(sem, inc=1, device_id={"tp": i}, device_id_type=MESH)
    if nd > 1:
        d = lax.axis_index("dp")

        def one(e, _):
            pl.semaphore_signal(sem, inc=1, device_id={"dp": (d + e) % nd, "tp": lax.axis_index("tp")}, device_id_type=MESH)
            return 0

        lax.fori_loop(1, nd, one, 0)
    pl.semaphore_wait(sem, len(ids) + nd - 1)


def _block(ref, d, nd, rows, cols):
    a = math.gcd(nd, 20)
    b = nd // a
    r, c = rows // a, cols // b
    return ref.at[pl.ds(pl.multiple_of((d // b) * r, 8), r), pl.ds(pl.multiple_of((d % b) * c, 128), c)]


class _Prefetch:
    def __init__(self, nz, nd, place, srcs, dsts, sems):
        self.nz, self.nd = nz, nd
        self.t, self.z, self.c = place
        self.d = lax.axis_index("dp")
        self.srcs, self.dsts = srcs, dsts
        self.ring_send, self.ring_recv, self.peer_send, self.peer_recv = sems

    def part(self, j, s, d):
        sign = 1 - 2 * j
        chip = _chip(self.z, self.c, self.nz, -sign, s) // 2
        ref = self.dsts[j].at[chip]
        return _block(ref, d, self.nd, ref.shape[0], ref.shape[1])

    def ring(self, j, s, first=False):
        if first:
            ref = self.srcs[j]
            src = _block(ref, self.d, self.nd, ref.shape[0], ref.shape[1])
        else:
            src = self.part(j, s, self.d)
        return pltpu.make_async_remote_copy(
            src_ref=src, dst_ref=self.part(j, s, self.d), send_sem=self.ring_send.at[j, s], recv_sem=self.ring_recv.at[j, s + 1],
            device_id={"tp": _chip(self.z, self.c, self.nz, 1 - 2 * j, 1)}, device_id_type=MESH)

    def peer(self, j, s, e):
        mine = self.part(j, s, self.d)
        return pltpu.make_async_remote_copy(
            src_ref=mine, dst_ref=mine, send_sem=self.peer_send.at[j, s, e], recv_sem=self.peer_recv.at[j, s, e],
            device_id={"dp": (self.d + e) % self.nd, "tp": self.t}, device_id_type=MESH)

    def start_ring(self):
        for j in (0, 1):
            self.ring(j, 0, True).start()

    def arrived(self, s):
        for j in (0, 1):
            self.ring(j, s - 1).wait_recv()

            @pl.when(s < self.nz - 1)
            def _():
                self.ring(j, s).start()

    def to_peers(self, s):
        def one(e, _):
            for j in (0, 1):
                self.peer(j, s, e).start()
            return 0

        lax.fori_loop(1, self.nd, one, 0)

    def drain_peers(self, lo, hi):
        def one(i, _):
            s, e = lo + i // (self.nd - 1), 1 + i % (self.nd - 1)
            for j in (0, 1):
                self.peer(j, s, e).wait()
            return 0

        lax.fori_loop(0, (hi - lo) * (self.nd - 1), one, 0)

    def drain_ring(self):
        def one(s, _):
            for j in (0, 1):
                self.ring(j, s).wait_send()
            return 0

        lax.fori_loop(0, self.nz - 1, one, 0)


def _ring_kernel(kind, layer, nz, nd, streams, names, *refs):
    r_ = dict(zip(names, refs, strict=True))
    (x_ref, g_ref, wa_ref, wb_ref, out_ref,
     abuf, pbuf, rbuf, wa, wb, own32, p32, mid, mid2,
     x_sem, w_sem, wsend_sem, wrecv_sem, ag_send, ag_recv, rs_send, rs_recv) = (r_[n] for n in (
         "x", "g", "wa", "wb", "out", "abuf", "pbuf", "rbuf", "wa_v", "wb_v", "own32", "p32", "mid", "mid2",
         "x_sem", "w_sem", "wsend", "wrecv", "ag_send", "ag_recv", "rs_send", "rs_recv"))
    gather = kind != "att0"
    attention = kind != "mlp"
    t, z, c = _place(nz)
    nxt = [_chip(z, c, nz, sg, 1) for _, _, sg in streams]
    peer = t + 1 - 2 * c
    rows, width = own32.shape
    last = nz - 1

    pre = None
    split = (nz + 1) // 2
    if "gq" in r_:
        pre = _Prefetch(nz, nd, (t, z, c), [r_[n].at[layer + 1] for n in ("pa", "pb") if n in r_], [r_["gq"], r_["go"]],
                        [r_[n] for n in ("pr_send", "pr_recv", "pp_send", "pp_recv")])
    _barrier([_chip(z, c, nz, 1, 1), _chip(z, c, nz, -1, 1), peer], nd if pre else 1)

    own_w, send_w = [], []
    for i, (src, dst) in enumerate(((wa_ref, wa), (wb_ref, wb))):
        src = src.at[layer]
        if kind == "mlp" and i == 0:
            n = src.shape[1]
            lo, hi = dst.at[:, pl.ds(0, n)], dst.at[:, pl.ds(n, n)]
        else:
            n = src.shape[0]
            lo, hi = dst.at[pl.ds(0, n)], dst.at[pl.ds(n, n)]
        own_w.append(pltpu.make_async_copy(src, lo, w_sem.at[i]))
        send_w.append(pltpu.make_async_remote_copy(
            src_ref=src, dst_ref=hi, send_sem=wsend_sem.at[i], recv_sem=wrecv_sem.at[i],
            device_id={"tp": peer}, device_id_type=MESH))

    def x_copy(k, s):
        r0, nr, sg = streams[k]
        dev = _chip(z, c, nz, -sg, s)
        src = x_ref.at[pl.ds(pl.multiple_of(dev * rows + r0, 32), nr)]
        return pltpu.make_async_copy(src, abuf.at[s, pl.ds(r0, nr)], x_sem.at[k, s])

    def ag_copy(k, s):
        r0, nr, _ = streams[k]
        r = pl.ds(r0, nr)
        return pltpu.make_async_remote_copy(
            src_ref=abuf.at[s, r], dst_ref=abuf.at[s + 1, r], send_sem=ag_send.at[k, s], recv_sem=ag_recv.at[k, s + 1],
            device_id={"tp": nxt[k]}, device_id_type=MESH)

    def rs_copy(k, s):
        r0, nr, _ = streams[k]
        r = pl.ds(r0, nr)
        return pltpu.make_async_remote_copy(
            src_ref=pbuf.at[s, r], dst_ref=rbuf.at[s, r], send_sem=rs_send.at[k, s], recv_sem=rs_recv.at[k, s],
            device_id={"tp": nxt[k]}, device_id_type=MESH)

    ks = range(len(streams))
    g = g_ref[pl.ds(layer, 1), :]
    if not gather:
        for i in range(nz):
            for k in ks:
                x_copy(k, (i + 1) % nz).start()
    if pre and not gather:
        pre.start_ring()
    for w in own_w + send_w:
        w.start()
    if gather:
        _ln_rows(lambda r: x_ref[r, :], lambda r, v: abuf.__setitem__((0, r), v), g, rows)
        for k in ks:
            ag_copy(k, 0).start()
        own32[...] = x_ref[...].astype(F32)
    for w in own_w:
        w.wait()
    for w in send_w:
        w.wait_recv()

    if attention:
        hd = wb.shape[0] // (2 * 2)
        key = lax.broadcasted_iota(jnp.int32, (rows, rows), 0)
        query = lax.broadcasted_iota(jnp.int32, (rows, rows), 1)
        seq = rows // 3
        visible = (key <= query) & (key // seq == query // seq)

    def partial_sum(s):
        if attention:
            mid[...] = _dot(wa[...], abuf[s], 1, 1).astype(BF16)

            def head(h, _):
                base = h * (3 * hd)
                q = mid[pl.ds(pl.multiple_of(base, 16), hd), :]
                k = mid[pl.ds(pl.multiple_of(base + hd, 16), hd), :]
                v = mid[pl.ds(pl.multiple_of(base + 2 * hd, 16), hd), :]
                sc = _dot(k, q, 0, 0) * (hd ** -0.5)
                sc = jnp.where(visible, sc, -jnp.inf)
                e = jnp.exp(sc - jnp.max(sc, axis=0, keepdims=True))
                p = (e / jnp.sum(e, axis=0, keepdims=True)).astype(BF16)
                mid2[pl.ds(pl.multiple_of(h * hd, 16), hd), :] = _dot(v, p, 1, 0).astype(BF16)
                return 0

            lax.fori_loop(0, 4, head, 0)
            tile = 512

            def cols(n, _):
                cc = pl.ds(pl.multiple_of(n * tile, tile), tile)
                p32[:, cc] = _dot(mid2[...], wb[:, cc], 0, 0)
                return 0

            lax.fori_loop(0, width // tile, cols, 0)
        else:
            t1, t2 = 256, 512

            def hidden(n, _):
                cc = pl.ds(pl.multiple_of(n * t1, t1), t1)
                mid[:, cc] = jax.nn.gelu(_dot(abuf[s], wa[:, cc], 1, 0), approximate=True).astype(BF16)
                return 0

            lax.fori_loop(0, mid.shape[1] // t1, hidden, 0)

            def cols(n, _):
                cc = pl.ds(pl.multiple_of(n * t2, t2), t2)
                p32[:, cc] = _dot(mid[...], wb[:, cc], 1, 0)
                return 0

            lax.fori_loop(0, width // t2, cols, 0)

    if pre and gather:
        lax.fori_loop(split, nz, lambda s, _: (pre.to_peers(s), 0)[1], 0)

    def step(i, _):
        s = i if gather else i + ((9 - i) // 8) * (1 - 2 * i)

        if gather:
            @pl.when(s > 0)
            def _():
                for k in ks:
                    ag_copy(k, s - 1).wait_recv()

                    @pl.when(s < last)
                    def _():
                        ag_copy(k, s).start()
        else:
            if pre:
                @pl.when(i > 0)
                def _():
                    pre.arrived(i)

                    @pl.when(i < split)
                    def _():
                        pre.to_peers(i)
            for k in ks:
                x_copy(k, s).wait()

            @pl.when(s == 0)
            def _():
                own32[...] = abuf[0].astype(F32)

            _ln_rows(lambda r: abuf[s, r], lambda r, v: abuf.__setitem__((s, r), v), g, rows)

        partial_sum(s)

        @pl.when(s == 0)
        def _():
            own32[...] += p32[...]

        @pl.when(s > 0)
        def _():
            for k in ks:
                r0, nr, _ = streams[k]
                r = pl.ds(r0, nr)

                @pl.when(s == 1)
                def _():
                    pbuf[s, r] = p32[r, :].astype(BF16)

                @pl.when(s > 1)
                def _():
                    rs_copy(k, s - 1).wait_recv()
                    pbuf[s, r] = (p32[r, :] + rbuf[s - 1, r].astype(F32)).astype(BF16)

                rs_copy(k, s).start()

        return 0

    lax.fori_loop(0, nz, step, 0)

    for k in ks:
        r0, nr, _ = streams[k]
        r = pl.ds(r0, nr)
        rs_copy(k, last).wait_recv()
        out_ref[r, :] = (own32[r, :] + rbuf[last, r].astype(F32)).astype(BF16)

    def drain(s, _):
        for k in ks:
            rs_copy(k, s).wait_send()
            if gather:
                ag_copy(k, s - 1).wait_send()
        return 0

    lax.fori_loop(1, nz, drain, 0)
    for w in send_w:
        w.wait_send()
    if pre:
        if gather:
            pre.drain_peers(split, nz)
        else:
            pre.drain_ring()
            pre.drain_peers(1, split)


def _ring_call(kind, layer, nz, nd, cid, x, g, wa, wb, rows, width, prefetch=False, gathered=None):
    fine = ((0, rows // 3, 1), (rows // 3, rows // 3, 1), (2 * rows // 3, rows // 6, -1), (5 * rows // 6, rows // 6, -1))
    coarse = ((0, 2 * rows // 3, 1), (2 * rows // 3, rows // 3, -1))
    streams = fine if kind == "att0" else coarse
    nk = len(streams)
    big = pltpu.VMEM((nz, rows, width), BF16)
    if kind == "mlp":
        wshape = ((width, 2 * wa.shape[2]), (2 * wb.shape[1], width))
        mids = ((rows, 2 * wa.shape[2]), (16, 128))
    else:
        wshape = ((2 * wa.shape[1], width), (2 * wb.shape[1], width))
        mids = ((2 * wa.shape[1], rows), (2 * wb.shape[1], rows))
    vmem, hbm = pl.BlockSpec(memory_space=pltpu.VMEM), pl.BlockSpec(memory_space=pl.ANY)
    dma = pltpu.SemaphoreType.DMA
    ins = [("x", x, hbm if kind == "att0" else vmem), ("g", g, vmem), ("wa", wa, hbm), ("wb", wb, hbm)]
    outs = [("out", jax.ShapeDtypeStruct((rows, width), BF16), vmem)]
    alias = {}
    if prefetch:
        ins += [("pa", wa, hbm), ("pb", wb, hbm)]
        outs += [("gq", jax.ShapeDtypeStruct((nz, *wa.shape[1:]), BF16), hbm), ("go", jax.ShapeDtypeStruct((nz, *wb.shape[1:]), BF16), hbm)]
    if gathered:
        for i, (n, a) in enumerate(zip(("gq", "go"), gathered)):
            alias[len(ins)] = len(outs)
            ins += [(n + "_in", a, hbm)]
            outs += [(n, jax.ShapeDtypeStruct(a.shape, a.dtype), hbm)]
    scratch = [
        ("abuf", big), ("pbuf", big), ("rbuf", big), ("wa_v", pltpu.VMEM(wshape[0], BF16)), ("wb_v", pltpu.VMEM(wshape[1], BF16)),
        ("own32", pltpu.VMEM((rows, width), F32)), ("p32", pltpu.VMEM((rows, width), F32)),
        ("mid", pltpu.VMEM(mids[0], BF16)), ("mid2", pltpu.VMEM(mids[1], BF16)),
        ("x_sem", dma((nk, nz))), ("w_sem", dma((2,))), ("wsend", dma((2,))), ("wrecv", dma((2,))),
        ("ag_send", dma((nk, nz))), ("ag_recv", dma((nk, nz))), ("rs_send", dma((nk, nz))), ("rs_recv", dma((nk, nz))),
    ]
    if prefetch or gathered:
        scratch += [("pr_send", dma((2, nz))), ("pr_recv", dma((2, nz))), ("pp_send", dma((2, nz, nd))), ("pp_recv", dma((2, nz, nd)))]
    names = [e[0] for e in ins + outs + scratch]
    res = pl.pallas_call(
        functools.partial(_ring_kernel, kind, layer, nz, nd, streams, names),
        out_shape=[e[1] for e in outs],
        in_specs=[e[2] for e in ins],
        out_specs=[e[2] for e in outs],
        scratch_shapes=[e[1] for e in scratch],
        input_output_aliases=alias,
        compiler_params=pltpu.CompilerParams(collective_id=cid, has_side_effects=True, vmem_limit_bytes=VMEM_LIMIT),
        name=f"{kind}_{layer}",
    )(*[e[1] for e in ins])
    return res if len(res) > 1 else res[0]


def _local_kernel(layer, nz, x_ref, g_ref, wa_ref, wb_ref, gq_ref, go_ref, out_ref,
                  abuf, pbuf, rbuf, wa, wb, own32, mid, ot, wa_sem, wb_sem, a_send, a_recv, p_send, p_recv):
    t, z, c = _place(nz)
    peer = t + 1 - 2 * c
    rows, width = out_ref.shape
    na, nb = wa_ref.shape[1], wb_ref.shape[1]
    hd = na // 6
    tiles = pbuf.shape[0]
    _barrier([peer])

    def load(j, chip, here=False):
        dst, ref, own, sem = ((wa, gq_ref, wa_ref, wa_sem), (wb, go_ref, wb_ref, wb_sem))[j]
        n = own.shape[1]
        src = own.at[layer] if here else ref.at[chip]
        return pltpu.make_async_copy(src, dst.at[pl.ds(pl.multiple_of(chip * n, 16), n)], sem.at[chip])

    def start(j, chip):
        @pl.when(chip == z)
        def _():
            load(j, chip, True).start()

        @pl.when(chip != z)
        def _():
            load(j, chip).start()

    for j in (0, 1):
        lax.fori_loop(0, nz, lambda chip, _: (start(j, chip), 0)[1], 0)
    g = g_ref[pl.ds(layer, 1), :]
    _ln_rows(lambda r: x_ref[r, :], lambda r, v: abuf.__setitem__((r, slice(None)), v), g, rows)
    swap = pltpu.make_async_remote_copy(
        src_ref=abuf.at[pl.ds(0, rows)], dst_ref=abuf.at[pl.ds(rows, rows)], send_sem=a_send, recv_sem=a_recv,
        device_id={"tp": peer}, device_id_type=MESH)
    swap.start()
    own32[...] = x_ref[...].astype(F32)
    swap.wait_recv()

    blk = 128
    seq = rows // 3
    key = lax.broadcasted_iota(jnp.int32, (blk, blk), 0)
    query = lax.broadcasted_iota(jnp.int32, (blk, blk), 1)
    visible = (key <= query) & (key // seq == query // seq)

    def pair(i, _):
        for k in (0, 1):
            load(0, 2 * i + k).wait()
        w = wa[pl.ds(pl.multiple_of(i * 2 * na, 16), 2 * na), :]
        mid[...] = _dot(w, abuf[...], 1, 1).astype(BF16)

        def head(h, _):
            base = h * (3 * hd)
            for b in range(2 * rows // blk):
                cc = pl.ds(b * blk, blk)
                q = mid[pl.ds(pl.multiple_of(base, 16), hd), cc]
                k = mid[pl.ds(pl.multiple_of(base + hd, 16), hd), cc]
                v = mid[pl.ds(pl.multiple_of(base + 2 * hd, 16), hd), cc]
                sc = _dot(k, q, 0, 0) * (hd ** -0.5)
                sc = jnp.where(visible, sc, -jnp.inf)
                e = jnp.exp(sc - jnp.max(sc, axis=0, keepdims=True))
                p = (e / jnp.sum(e, axis=0, keepdims=True)).astype(BF16)
                ot[pl.ds(pl.multiple_of(i * 2 * nb + h * hd, 16), hd), cc] = _dot(v, p, 1, 0).astype(BF16)
            return 0

        lax.fori_loop(0, 4, head, 0)
        return 0

    lax.fori_loop(0, nz // 2, pair, 0)
    lax.fori_loop(0, nz, lambda chip, _: (load(1, chip).wait(), 0)[1], 0)

    def part(n):
        return pltpu.make_async_remote_copy(
            src_ref=pbuf.at[n], dst_ref=rbuf.at[n], send_sem=p_send.at[n], recv_sem=p_recv.at[n],
            device_id={"tp": peer}, device_id_type=MESH)

    tile = width // tiles

    def cols(n, _):
        cc = pl.ds(pl.multiple_of(n * tile, tile), tile)
        p = _dot(ot[...], wb[:, cc], 0, 0)
        pbuf[n] = p[rows:].astype(BF16)
        part(n).start()
        own32[:, cc] += p[:rows]
        return 0

    lax.fori_loop(0, tiles, cols, 0)

    def last(n, _):
        cc = pl.ds(pl.multiple_of(n * tile, tile), tile)
        part(n).wait()
        out_ref[:, cc] = (own32[:, cc] + rbuf[n].astype(F32)).astype(BF16)
        return 0

    lax.fori_loop(0, tiles, last, 0)
    swap.wait_send()


def _local_call(layer, nz, cid, x, g, wa, wb, gq, go):
    rows, width = x.shape
    na, nb = wa.shape[1], wb.shape[1]
    tiles = 5
    vmem, hbm = pl.BlockSpec(memory_space=pltpu.VMEM), pl.BlockSpec(memory_space=pl.ANY)
    dma = pltpu.SemaphoreType.DMA
    return pl.pallas_call(
        functools.partial(_local_kernel, layer, nz),
        out_shape=jax.ShapeDtypeStruct((rows, width), BF16),
        in_specs=[vmem, vmem, hbm, hbm, hbm, hbm],
        out_specs=vmem,
        scratch_shapes=[
            pltpu.VMEM((2 * rows, width), BF16), pltpu.VMEM((tiles, rows, width // tiles), BF16),
            pltpu.VMEM((tiles, rows, width // tiles), BF16),
            pltpu.VMEM((nz * na, width), BF16), pltpu.VMEM((nz * nb, width), BF16), pltpu.VMEM((rows, width), F32),
            pltpu.VMEM((2 * na, 2 * rows), BF16), pltpu.VMEM((nz * nb, 2 * rows), BF16),
            dma((nz,)), dma((nz,)), dma, dma, dma((tiles,)), dma((tiles,)),
        ],
        compiler_params=pltpu.CompilerParams(collective_id=cid, has_side_effects=True, vmem_limit_bytes=VMEM_LIMIT),
        name=f"local_{layer}",
    )(x, g, wa, wb, gq, go)


def _gather_kernel(nz, streams, x_ref, out_ref, buf, loc_sem, send_sem, recv_sem, psend_sem, precv_sem):
    t, z, c = _place(nz)
    nxt = [_chip(z, c, nz, sg, 1) for _, _, sg in streams]
    peer = t + 1 - 2 * c
    rows = x_ref.shape[0]
    ks = range(len(streams))
    last = nz - 1
    _barrier([_chip(z, c, nz, 1, 1), _chip(z, c, nz, -1, 1), peer])

    def src(k, s):
        r0, nr, _ = streams[k]
        return buf.at[s, pl.ds(r0, nr)]

    def spot(k, s, core):
        r0, nr, sg = streams[k]
        dev = _chip(z, core, nz, -sg * (1 - 2 * c) * (1 - 2 * core), s)
        return out_ref.at[pl.ds(pl.multiple_of(dev * rows + r0, 32), nr)]

    def ring(k, s):
        return pltpu.make_async_remote_copy(
            src_ref=src(k, s), dst_ref=src(k, s + 1), send_sem=send_sem.at[k, s], recv_sem=recv_sem.at[k, s + 1],
            device_id={"tp": nxt[k]}, device_id_type=MESH)

    def local(k, s):
        return pltpu.make_async_copy(src(k, s), spot(k, s, c), loc_sem.at[k, s])

    def across(k, s):
        return pltpu.make_async_remote_copy(
            src_ref=src(k, s), dst_ref=spot(k, s, c), send_sem=psend_sem.at[k, s], recv_sem=precv_sem.at[k, s],
            device_id={"tp": peer}, device_id_type=MESH)

    own = pltpu.make_async_copy(x_ref, buf.at[0], loc_sem.at[0, 0])
    own.start()
    own.wait()
    for k in ks:
        ring(k, 0).start()
    for k in ks:
        local(k, 0).start()
        across(k, 0).start()

    def step(s, _):
        for k in ks:
            ring(k, s - 1).wait_recv()

            @pl.when(s < last)
            def _():
                ring(k, s).start()

            local(k, s).start()
            across(k, s).start()
        return 0

    lax.fori_loop(1, nz, step, 0)

    def drain(s, _):
        for k in ks:
            local(k, s).wait()
            across(k, s).wait()

            @pl.when(s < last)
            def _():
                ring(k, s).wait_send()
        return 0

    lax.fori_loop(0, nz, drain, 0)


def _gather_call(nz, cid, x):
    rows, width = x.shape
    streams = ((0, rows // 3, 1), (rows // 3, rows // 3, 1), (2 * rows // 3, rows // 6, -1), (5 * rows // 6, rows // 6, -1))
    nk = len(streams)
    dma = pltpu.SemaphoreType.DMA
    hbm = pl.BlockSpec(memory_space=pl.ANY)
    return pl.pallas_call(
        functools.partial(_gather_kernel, nz, streams),
        out_shape=jax.ShapeDtypeStruct((2 * nz * rows, width), BF16),
        in_specs=[hbm],
        out_specs=hbm,
        scratch_shapes=[pltpu.VMEM((nz, rows, width), BF16)] + [dma((nk, nz))] * 5,
        compiler_params=pltpu.CompilerParams(collective_id=cid, has_side_effects=True, vmem_limit_bytes=VMEM_LIMIT),
        name="gather",
    )(x)


def solution(mesh):
    n = mesh.shape["tp"]
    nz = n // 2
    nd = mesh.shape["dp"]

    def body(x, g1, g2, wqkv, wo, w1, w2):
        b, s, d = x.shape
        rows = b * s // n
        layers, _, hl, hd3 = wqkv.shape
        wt = wqkv.transpose(0, 2, 3, 1).reshape(layers, hl * hd3, d)
        h = x.reshape(b * s, d)
        h, gq, go = _ring_call("att0", 0, nz, nd, 0, h, g1, wt, wo, rows, d, prefetch=True)
        h, gq, go = _ring_call("mlp", 0, nz, nd, 1, h, g2, w1, w2, rows, d, gathered=(gq, go))
        h = _local_call(1, nz, 2, h, g1, wt, wo, gq, go)
        h = _ring_call("mlp", 1, nz, nd, 3, h, g2, w1, w2, rows, d)
        cid = 4
        return _gather_call(nz, cid, h).reshape(b, s, d)

    in_specs = (P("dp"), P(), P(), P(None, None, "tp", None), P(None, "tp", None), P(None, None, "tp"), P(None, "tp", None))
    return jax.shard_map(body, mesh=mesh, in_specs=in_specs, out_specs=P("dp"), check_vma=False)
```

```python
import functools
import math

import jax
import jax.numpy as jnp
from jax import lax
from jax.experimental import pallas as pl
from jax.experimental.pallas import tpu as pltpu
from jax.sharding import PartitionSpec as P

EPS = 1e-5
MESH = pl.DeviceIdType.MESH
F32 = jnp.float32
BF16 = jnp.bfloat16
VMEM_LIMIT = 63 * 1024 * 1024


def _dot(a, b, ca, cb):
    return lax.dot_general(a, b, (((ca,), (cb,)), ((), ())), preferred_element_type=F32)


def _ln_rows(load, store, g, rows):
    def body(i, _):
        r = pl.ds(pl.multiple_of(i * 16, 16), 16)
        xf = load(r).astype(F32)
        d = xf - jnp.mean(xf, axis=-1, keepdims=True)
        var = jnp.mean(d * d, axis=-1, keepdims=True)
        store(r, (d * lax.rsqrt(var + EPS) * g).astype(BF16))
        return 0

    lax.fori_loop(0, rows // 16, body, 0)


def _place(nz):
    t = lax.axis_index("tp")
    z, c = t // 2, t % 2
    return t, z, c


def _chip(z, c, nz, sign, steps):
    fwd = sign * (1 - 2 * c) * steps
    return ((z + fwd + 8 * nz) % nz) * 2 + c


def _barrier(ids, nd=1):
    sem = pltpu.get_barrier_semaphore()
    for i in ids:
        pl.semaphore_signal(sem, inc=1, device_id={"tp": i}, device_id_type=MESH)
    if nd > 1:
        d = lax.axis_index("dp")

        def one(e, _):
            pl.semaphore_signal(sem, inc=1, device_id={"dp": (d + e) % nd, "tp": lax.axis_index("tp")}, device_id_type=MESH)
            return 0

        lax.fori_loop(1, nd, one, 0)
    pl.semaphore_wait(sem, len(ids) + nd - 1)


def _block(ref, d, nd, rows, cols):
    a = math.gcd(nd, 20)
    b = nd // a
    r, c = rows // a, cols // b
    return ref.at[pl.ds(pl.multiple_of((d // b) * r, 8), r), pl.ds(pl.multiple_of((d % b) * c, 128), c)]


class _Prefetch:
    def __init__(self, nz, nd, place, srcs, dsts, sems):
        self.nz, self.nd = nz, nd
        self.t, self.z, self.c = place
        self.d = lax.axis_index("dp")
        self.srcs, self.dsts = srcs, dsts
        self.ring_send, self.ring_recv, self.peer_send, self.peer_recv = sems

    def part(self, j, s, d):
        sign = 1 - 2 * j
        chip = _chip(self.z, self.c, self.nz, -sign, s) // 2
        ref = self.dsts[j].at[chip]
        return _block(ref, d, self.nd, ref.shape[0], ref.shape[1])

    def ring(self, j, s, first=False):
        if first:
            ref = self.srcs[j]
            src = _block(ref, self.d, self.nd, ref.shape[0], ref.shape[1])
        else:
            src = self.part(j, s, self.d)
        return pltpu.make_async_remote_copy(
            src_ref=src, dst_ref=self.part(j, s, self.d), send_sem=self.ring_send.at[j, s], recv_sem=self.ring_recv.at[j, s + 1],
            device_id={"tp": _chip(self.z, self.c, self.nz, 1 - 2 * j, 1)}, device_id_type=MESH)

    def peer(self, j, s, e):
        mine = self.part(j, s, self.d)
        return pltpu.make_async_remote_copy(
            src_ref=mine, dst_ref=mine, send_sem=self.peer_send.at[j, s, e], recv_sem=self.peer_recv.at[j, s, e],
            device_id={"dp": (self.d + e) % self.nd, "tp": self.t}, device_id_type=MESH)

    def start_ring(self):
        for j in (0, 1):
            self.ring(j, 0, True).start()

    def arrived(self, s):
        for j in (0, 1):
            self.ring(j, s - 1).wait_recv()

            @pl.when(s < self.nz - 1)
            def _():
                self.ring(j, s).start()

    def to_peers(self, s):
        def one(e, _):
            for j in (0, 1):
                self.peer(j, s, e).start()
            return 0

        lax.fori_loop(1, self.nd, one, 0)

    def drain_peers(self, lo, hi):
        def one(i, _):
            s, e = lo + i // (self.nd - 1), 1 + i % (self.nd - 1)
            for j in (0, 1):
                self.peer(j, s, e).wait()
            return 0

        lax.fori_loop(0, (hi - lo) * (self.nd - 1), one, 0)

    def drain_ring(self):
        def one(s, _):
            for j in (0, 1):
                self.ring(j, s).wait_send()
            return 0

        lax.fori_loop(0, self.nz - 1, one, 0)


def _kernel(nz, nd, names, *refs):
    R = dict(zip(names, refs, strict=True))
    x_ref, g1_ref, g2_ref, wt_ref, wo_ref, w1_ref, w2_ref, out_ref = (
        R[n] for n in ("x", "g1", "g2", "wt", "wo", "w1", "w2", "out"))
    abuf, pbuf, rbuf, wa, wb, lw, lo, la, own32, p32, mid, hid, ot, tsend, trecv = (
        R[n] for n in ("abuf", "pbuf", "rbuf", "wa", "wb", "lw", "lo", "la", "own32", "p32", "mid", "hid", "ot", "tsend", "trecv"))
    t, z, c = _place(nz)
    peer = t + 1 - 2 * c
    rows, width = own32.shape
    na, nb = wt_ref.shape[1], wo_ref.shape[1]
    ff = w1_ref.shape[2]
    hd = na // 6
    seq = rows // 3
    last = nz - 1
    streams = ((0, seq, 1), (seq, seq, 1), (2 * seq, seq // 2, -1), (2 * seq + seq // 2, seq // 2, -1))
    ks = range(len(streams))
    nxt = [_chip(z, c, nz, sg, 1) for _, _, sg in streams]
    pre = _Prefetch(nz, nd, (t, z, c), [wt_ref.at[1], wo_ref.at[1]], [R["gq"], R["go"]],
                    [R[n] for n in ("pr_send", "pr_recv", "pp_send", "pp_recv")])

    def to_peer(src, dst, send, recv):
        return pltpu.make_async_remote_copy(
            src_ref=src, dst_ref=dst, send_sem=send, recv_sem=recv, device_id={"tp": peer}, device_id_type=MESH)

    def at(buf, s, r0, n):
        return buf.at[pl.ds(pl.multiple_of(s * rows + r0, 32), n)]

    def rd(s, r0, n):
        return pl.ds(pl.multiple_of(s * rows + r0, 32), n)

    def loop(lo_, hi_, f):
        lax.fori_loop(lo_, hi_, lambda i, _: (f(i), 0)[1], 0)

    def weight(i, l, across=False):
        src, lo_, hi_ = (
            (wt_ref, lw.at[pl.ds(0, na)], lw.at[pl.ds(na, na)]),
            (wo_ref, lo.at[pl.ds(0, nb)], lo.at[pl.ds(nb, nb)]),
            (w1_ref, wa.at[:, pl.ds(0, ff)], wa.at[:, pl.ds(ff, ff)]),
            (w2_ref, wb.at[pl.ds(0, ff)], wb.at[pl.ds(ff, ff)]),
        )[i]
        j = i + 2 * l
        if across:
            return to_peer(src.at[l], hi_, R["wsend"].at[j], R["wrecv"].at[j])
        return pltpu.make_async_copy(src.at[l], lo_, R["w_sem"].at[j])

    def x_copy(k, s):
        r0, nr, sg = streams[k]
        dev = _chip(z, c, nz, -sg, s)
        return pltpu.make_async_copy(at(x_ref, dev, r0, nr), at(abuf, s, r0, nr), R["x_sem"].at[k, s])

    def ag_copy(ph, k, s):
        r0, nr, _ = streams[k]
        return pltpu.make_async_remote_copy(
            src_ref=at(abuf, s, r0, nr), dst_ref=at(abuf, s + 1, r0, nr),
            send_sem=R["ag_send"].at[ph, k, s], recv_sem=R["ag_recv"].at[ph, k, s + 1],
            device_id={"tp": nxt[k]}, device_id_type=MESH)

    def rs_copy(ph, k, s):
        r0, nr, _ = streams[k]
        return pltpu.make_async_remote_copy(
            src_ref=at(pbuf, s, r0, nr), dst_ref=at(rbuf, s, r0, nr),
            send_sem=R["rs_send"].at[ph, k, s], recv_sem=R["rs_recv"].at[ph, k, s],
            device_id={"tp": nxt[k]}, device_id_type=MESH)

    def normalise(g, r0, n):
        def load(r):
            return own32[pl.ds(pl.multiple_of(r0 + r.start, 16), 16), :]

        def store(r, v):
            abuf[pl.ds(pl.multiple_of(r0 + r.start, 16), 16), :] = v

        _ln_rows(load, store, g, n)

    def reduce_step(ph, s):
        for k in ks:
            r0, nr, _ = streams[k]

            @pl.when(s == 1)
            def _():
                pbuf[rd(s, r0, nr), :] = p32[pl.ds(r0, nr), :].astype(BF16)

            @pl.when(s > 1)
            def _():
                rs_copy(ph, k, s - 1).wait_recv()
                pbuf[rd(s, r0, nr), :] = (p32[pl.ds(r0, nr), :] + rbuf[rd(s - 1, r0, nr), :].astype(F32)).astype(BF16)

            rs_copy(ph, k, s).start()

    def finish(ph, k):
        r0, nr, _ = streams[k]
        rs_copy(ph, k, last).wait_recv()
        v = (own32[pl.ds(r0, nr), :] + rbuf[rd(last, r0, nr), :].astype(F32)).astype(BF16)
        own32[pl.ds(r0, nr), :] = v.astype(F32)
        return v

    def mlp(s):
        t1, t2 = 256, 512

        def hidden(n):
            cc = pl.ds(pl.multiple_of(n * t1, t1), t1)
            hid[:, cc] = jax.nn.gelu(_dot(abuf[rd(s, 0, rows), :], wa[:, cc], 1, 0), approximate=True).astype(BF16)

        loop(0, 2 * ff // t1, hidden)

        def cols(n):
            cc = pl.ds(pl.multiple_of(n * t2, t2), t2)
            p32[:, cc] = _dot(hid[...], wb[:, cc], 1, 0)

        loop(0, width // t2, cols)

    def mask(n):
        key = lax.broadcasted_iota(jnp.int32, (n, n), 0)
        query = lax.broadcasted_iota(jnp.int32, (n, n), 1)
        return (key <= query) & (key // seq == query // seq)

    def head(base, cc, visible):
        q = mid[pl.ds(pl.multiple_of(base, 16), hd), cc]
        k = mid[pl.ds(pl.multiple_of(base + hd, 16), hd), cc]
        v = mid[pl.ds(pl.multiple_of(base + 2 * hd, 16), hd), cc]
        sc = jnp.where(visible, _dot(k, q, 0, 0) * (hd ** -0.5), -jnp.inf)
        e = jnp.exp(sc - jnp.max(sc, axis=0, keepdims=True))
        p = (e / jnp.sum(e, axis=0, keepdims=True)).astype(BF16)
        return _dot(v, p, 1, 0).astype(BF16)

    def attend_all(s, visible):
        mid[:, pl.ds(0, rows)] = _dot(lw[pl.ds(0, 2 * na), :], abuf[rd(s, 0, rows), :], 1, 1).astype(BF16)

        def one(h):
            ot[pl.ds(pl.multiple_of(h * hd, 16), hd), pl.ds(0, rows)] = head(h * (3 * hd), pl.ds(0, rows), visible)

        loop(0, 4, one)
        tile = 512

        def cols(n):
            cc = pl.ds(pl.multiple_of(n * tile, tile), tile)
            p32[:, cc] = _dot(ot[pl.ds(0, 2 * nb), pl.ds(0, rows)], lo[pl.ds(0, 2 * nb), cc], 0, 0)

        loop(0, width // tile, cols)

    _barrier([_chip(z, c, nz, 1, 1), _chip(z, c, nz, -1, 1), peer], nd)

    for i in range(nz):
        for k in ks:
            x_copy(k, (i + 1) % nz).start()
    pre.start_ring()
    for i in range(4):
        weight(i, 0).start()
        weight(i, 0, True).start()
    for i in (0, 1):
        weight(i, 0).wait()
        weight(i, 0, True).wait_recv()
    visible = mask(rows)
    g = g1_ref[pl.ds(0, 1), :]

    def att_step(i):
        s = i + ((9 - i) // 8) * (1 - 2 * i)

        @pl.when(i > 0)
        def _():
            pre.arrived(i)
            pre.to_peers(i)

        for k in ks:
            x_copy(k, s).wait()

        @pl.when(s == 0)
        def _():
            own32[...] = abuf[pl.ds(0, rows), :].astype(F32)

        def load(r):
            return abuf[pl.ds(pl.multiple_of(s * rows + r.start, 16), 16), :]

        def store(r, v):
            abuf[pl.ds(pl.multiple_of(s * rows + r.start, 16), 16), :] = v

        _ln_rows(load, store, g, rows)
        attend_all(s, visible)

        @pl.when(s == 0)
        def _():
            own32[...] += p32[...]

        @pl.when(s > 0)
        def _():
            reduce_step(0, s)

    loop(0, nz, att_step)

    def mlp_phase(l):
        for i in (2, 3):
            weight(i, l).wait()
            weight(i, l, True).wait_recv()

        def step(s):
            @pl.when(s > 0)
            def _():
                for k in ks:
                    ag_copy(l, k, s - 1).wait_recv()

                    @pl.when(s < last)
                    def _():
                        ag_copy(l, k, s).start()

            mlp(s)

            @pl.when(s == 0)
            def _():
                own32[...] += p32[...]

            @pl.when(s > 0)
            def _():
                reduce_step(1 + l, s)

        loop(0, nz, step)

    def drain_rs(ph):
        loop(1, nz, lambda s: [rs_copy(ph, k, s).wait_send() for k in ks])

    def drain_ag(ph):
        loop(0, last, lambda s: [ag_copy(ph, k, s).wait_send() for k in ks])

    def release(ph):
        drain_ag(ph)
        for sg in (1, -1):
            pl.semaphore_signal(R["free"].at[ph], inc=1, device_id={"tp": _chip(z, c, nz, sg, 1)}, device_id_type=MESH)

    g = g2_ref[pl.ds(0, 1), :]
    for k in ks:
        finish(0, k)
        normalise(g, streams[k][0], streams[k][1])
        ag_copy(0, k, 0).start()
    drain_rs(0)
    mlp_phase(0)

    def shard(j, chip, here=False):
        dst, ref, own, sem, n, slots = ((lw, R["gq"], wt_ref, R["lw_sem"], na, 4), (lo, R["go"], wo_ref, R["lo_sem"], nb, nz))[j]
        d = dst.at[pl.ds(pl.multiple_of((chip % slots) * n, 16), n)]
        return pltpu.make_async_copy(own.at[1] if here else ref.at[chip], d, sem.at[chip])

    def start_shard(j, chip):
        @pl.when(chip == z)
        def _():
            shard(j, chip, True).start()

        @pl.when(chip != z)
        def _():
            shard(j, chip).start()

    pre.drain_ring()
    pre.drain_peers(1, nz)
    loop(0, 4, lambda chip: start_shard(0, chip))
    loop(0, nz, lambda chip: start_shard(1, chip))
    g = g1_ref[pl.ds(1, 1), :]
    for i in range(4):
        weight(i, 0, True).wait_send()
    ready = R["ready"]
    pl.semaphore_signal(ready, inc=1, device_id={"tp": peer}, device_id_type=MESH)
    for k in ks:
        finish(1, k)
        r0, nr, _ = streams[k]

        def load(r, r0=r0):
            return own32[pl.ds(pl.multiple_of(r0 + r.start, 16), 16), :]

        def store(r, v, r0=r0):
            la[pl.ds(pl.multiple_of(r0 + r.start, 16), 16), :] = v

        _ln_rows(load, store, g, nr)
    pl.semaphore_wait(ready, 1)
    swap = to_peer(la.at[pl.ds(0, rows)], la.at[pl.ds(rows, rows)], R["a_send"], R["a_recv"])
    swap.start()
    for i in (2, 3):
        weight(i, 1).start()
        weight(i, 1, True).start()
    drain_rs(1)
    release(0)
    swap.wait_recv()
    blk = 2 * seq
    visible = mask(blk)

    def pair(i):
        for k in (0, 1):
            shard(0, 2 * i + k).wait()
        w = lw[pl.ds(pl.multiple_of((i % 2) * 2 * na, 16), 2 * na), :]
        mid[...] = _dot(w, la[...], 1, 1).astype(BF16)

        @pl.when(i < nz // 2 - 2)
        def _():
            for k in (0, 1):
                start_shard(0, 2 * i + 4 + k)

        def one(h):
            for b in range(2 * rows // blk):
                cc = pl.ds(b * blk, blk)
                ot[pl.ds(pl.multiple_of(i * 2 * nb + h * hd, 16), hd), cc] = head(h * (3 * hd), cc, visible)

        loop(0, 4, one)

    loop(0, nz // 2, pair)
    loop(0, nz, lambda chip: shard(1, chip).wait())
    tiles = tsend.shape[0]
    tile = width // tiles

    def part(n):
        return to_peer(tsend.at[n], trecv.at[n], R["p_send"].at[n], R["p_recv"].at[n])

    def cols(n):
        cc = pl.ds(pl.multiple_of(n * tile, tile), tile)
        p = _dot(ot[...], lo[:, cc], 0, 0)
        tsend[n] = p[rows:].astype(BF16)
        part(n).start()
        own32[:, cc] += p[:rows]

    loop(0, tiles, cols)

    def add_part(n):
        cc = pl.ds(pl.multiple_of(n * tile, tile), tile)
        part(n).wait()
        own32[:, cc] = (own32[:, cc] + trecv[n].astype(F32)).astype(BF16).astype(F32)

    loop(0, tiles, add_part)
    swap.wait_send()

    g = g2_ref[pl.ds(1, 1), :]
    pl.semaphore_wait(R["free"].at[0], 2)
    for k in ks:
        normalise(g, streams[k][0], streams[k][1])
        ag_copy(1, k, 0).start()
    mlp_phase(1)

    def spot(k, s):
        r0, nr, sg = streams[k]
        return at(out_ref, _chip(z, c, nz, -sg, s), r0, nr)

    def local(k, s):
        r0, nr, _ = streams[k]
        return pltpu.make_async_copy(at(abuf, s, r0, nr), spot(k, s), R["o_sem"].at[k, s])

    def across(k, s):
        r0, nr, _ = streams[k]
        return to_peer(at(abuf, s, r0, nr), spot(k, s), R["o_send"].at[k, s], R["o_recv"].at[k, s])

    release(1)
    for k in ks:
        r0, nr, _ = streams[k]
        abuf[pl.ds(r0, nr), :] = finish(2, k)
        if k == 0:
            pl.semaphore_wait(R["free"].at[1], 2)
        ag_copy(2, k, 0).start()
    for k in ks:
        local(k, 0).start()
        across(k, 0).start()
    drain_rs(2)
    for i in (2, 3):
        weight(i, 1, True).wait_send()

    def out_step(s):
        for k in ks:
            ag_copy(2, k, s - 1).wait_recv()

            @pl.when(s < last)
            def _():
                ag_copy(2, k, s).start()

            local(k, s).start()
            across(k, s).start()

    loop(1, nz, out_step)
    drain_ag(2)

    def drain_out(s):
        for k in ks:
            local(k, s).wait()
            across(k, s).wait()

    loop(0, nz, drain_out)


def _call(nz, nd, x, g1, g2, wt, wo, w1, w2):
    tokens, width = x.shape
    rows = tokens // (2 * nz)
    na, nb, ff = wt.shape[1], wo.shape[1], w1.shape[2]
    nk, tiles = 4, 5
    vmem, hbm = pl.BlockSpec(memory_space=pltpu.VMEM), pl.BlockSpec(memory_space=pl.ANY)
    dma = pltpu.SemaphoreType.DMA
    ins = [("x", x, hbm), ("g1", g1, vmem), ("g2", g2, vmem), ("wt", wt, hbm), ("wo", wo, hbm), ("w1", w1, hbm), ("w2", w2, hbm)]
    outs = [("out", x.shape), ("gq", (nz, na, width)), ("go", (nz, nb, width))]
    vm = [("abuf", (nz * rows, width)), ("pbuf", (nz * rows, width)), ("rbuf", (nz * rows, width)),
          ("wa", (width, 2 * ff)), ("wb", (2 * ff, width)), ("lw", (4 * na, width)), ("lo", (nz * nb, width)),
          ("la", (2 * rows, width)), ("mid", (2 * na, 2 * rows)), ("hid", (rows, 2 * ff)), ("ot", (nz * nb, 2 * rows)),
          ("tsend", (tiles, rows, width // tiles)), ("trecv", (tiles, rows, width // tiles))]
    sems = [("x_sem", (nk, nz)), ("w_sem", (6,)), ("wsend", (6,)), ("wrecv", (6,)),
            ("ag_send", (3, nk, nz)), ("ag_recv", (3, nk, nz)), ("rs_send", (3, nk, nz)), ("rs_recv", (3, nk, nz)),
            ("pr_send", (2, nz)), ("pr_recv", (2, nz)), ("pp_send", (2, nz, nd)), ("pp_recv", (2, nz, nd)),
            ("lw_sem", (nz,)), ("lo_sem", (nz,)), ("a_send", ()), ("a_recv", ()), ("p_send", (tiles,)), ("p_recv", (tiles,)),
            ("o_sem", (nk, nz)), ("o_send", (nk, nz)), ("o_recv", (nk, nz))]
    scratch = [(n, pltpu.VMEM(sh, BF16)) for n, sh in vm]
    scratch += [("own32", pltpu.VMEM((rows, width), F32)), ("p32", pltpu.VMEM((rows, width), F32))]
    scratch += [(n, dma(sh) if sh else dma) for n, sh in sems] + [("ready", pltpu.SemaphoreType.REGULAR), ("free", pltpu.SemaphoreType.REGULAR((2,)))]
    names = [e[0] for e in ins + outs + scratch]
    return pl.pallas_call(
        functools.partial(_kernel, nz, nd, names),
        out_shape=[jax.ShapeDtypeStruct(sh, BF16) for _, sh in outs],
        in_specs=[e[2] for e in ins],
        out_specs=[hbm] * len(outs),
        scratch_shapes=[e[1] for e in scratch],
        compiler_params=pltpu.CompilerParams(collective_id=0, has_side_effects=True, vmem_limit_bytes=VMEM_LIMIT),
        name="layers",
    )(*[e[1] for e in ins])[0]


def solution(mesh):
    n = mesh.shape["tp"]

    def body(x, g1, g2, wqkv, wo, w1, w2):
        b, s, d = x.shape
        layers, _, hl, hd3 = wqkv.shape
        wt = wqkv.transpose(0, 2, 3, 1).reshape(layers, hl * hd3, d)
        return _call(n // 2, mesh.shape["dp"], x.reshape(b * s, d), g1, g2, wt, wo, w1, w2).reshape(b, s, d)

    in_specs = (P("dp"), P(), P(), P(None, None, "tp", None), P(None, "tp", None), P(None, None, "tp"), P(None, "tp", None))
    return jax.shard_map(body, mesh=mesh, in_specs=in_specs, out_specs=P("dp"), check_vma=False)
```
